256 devices in a mesh: rep: 2 (over z), exp: 128 (over x, y, core).
Axes of the slice: x: 8, y: 8, z: 2, core: 2. Of those that a mesh axis runs over, the one named last changes fastest.
The devices are a block of a 8x8x16 slice.
Arguments:
- a_tokens: bfloat16 [512, 7168], P(('rep', 'exp')), parts along dimension 0, may hold values from -6 to 6
- a_gain: float32 [7168], replicated, may hold values from 0.25 to 1.75
- dense_gate: bfloat16 [7168, 18432], P(None, 'exp'), may hold values from -0.0625 to 0.0625
- dense_up: bfloat16 [7168, 18432], P(None, 'exp'), may hold values from -0.0625 to 0.0625
- dense_down: bfloat16 [18432, 7168], P('exp'), may hold values from -0.046875 to 0.046875
- b_tokens: bfloat16 [1024, 7168], P(('rep', 'exp')), parts along dimension 0, may hold values from -6 to 6
- b_gain: float32 [7168], replicated, may hold values from 0.25 to 1.75
- expert_ids: int32 [1024, 8], P(('rep', 'exp')), parts along dimension 0, may hold values from 0 to 15, all different within a row; in each aligned block of 4 rows (0 to 3, 4 to 7, ...) at most 3 rows name the same one
- route_weights: float32 [1024, 8], P(('rep', 'exp')), parts along dimension 0, may hold values from 0.05 to 0.5
- expert_gate: bfloat16 [128, 7168, 128], P('exp'), may hold values from -0.0625 to 0.0625
- expert_up: bfloat16 [128, 7168, 128], P('exp'), may hold values from -0.0625 to 0.0625
- expert_down: bfloat16 [128, 128, 7168], P('exp'), may hold values from -0.1875 to 0.1875
Outputs:
- a_out: bfloat16 [512, 7168], P(('rep', 'exp')), parts along dimension 0
- b_out: bfloat16 [1024, 7168], P(('rep', 'exp')), parts along dimension 0
The draws below stay inside these ranges and needn't reach their ends.
There are 2 independent parts, one for each index of `rep`. The reference program is written for one: setup_inputs(seed, part) draws one part's arguments, and reference() takes and returns one part's arrays. A program takes and returns all parts, laid end to end along the dimension named above; an argument that names none is the same for every part. Nothing has to cross between parts.
Inputs may be any that keep to these rules, and one draw needn't show every extreme that they name: `expert_ids`: each row names 8 different experts. Among the rows of one device no expert is named more than 3 times, and in some devices one expert is named exactly 3 times.
All inputs are finite; a program needn't handle non-finite values.
Results may differ from the reference program's by a relative error of at most 0.008.
Values may be sent and summed in bfloat16 or wider, within the bound.
A program may use at most 128 MiB of HBM per device.

```python
import math
import jax
import jax.numpy as jnp
import numpy as np
from jax import lax

D = 7168
FF = 18432
EH = 1024
EXPERTS = 16
TOPK = 8
TB_DEV = 4
TA = 256
TB = 512
GROUP = 8
ES = 128
CAP = 3


def levels(stream_key, extent, pieces, low, high):
    def one(position, parts):
        draws = jax.random.uniform(jax.random.fold_in(jax.random.fold_in(stream_key, 6), position), (parts,), jnp.float32, low / len(pieces), high / len(pieces))
        return jnp.repeat(jnp.exp(draws), extent[position] // parts).reshape((-1,) + (1,) * (len(extent) - position - 1))

    level = one(*pieces[0])
    for cut in pieces[1:]:
        level = level * one(*cut)
    return level


def shared_out(stream_key, own, number, rows, amount, top, bound, slope):
    order = jax.random.permutation(stream_key, amount)
    packed, ordinary = load_shares(amount, rows * top, bound, slope, True), load_shares(amount, rows * top, bound, slope, False)
    places = jnp.arange(amount)

    def named(sizes, offset_by):
        used = int((sizes > 0).sum())
        fixed = max(1, used // 4)
        shifted = fixed + (places - fixed + offset_by * (used - fixed)) % max(1, amount - fixed)
        return jnp.zeros((amount,), jnp.int32).at[order[jnp.where(places < fixed, places, shifted)]].set(jnp.asarray(sizes, jnp.int32))

    sizes = jnp.where(number % 4 == 0, named(packed, number // 4), named(ordinary, number - number // 4 - 1))
    mixed = jax.random.permutation(jax.random.fold_in(own, 3), amount)
    donor, receiver = mixed[0:amount // 2 * 2:2], mixed[1:amount // 2 * 2:2]
    slack = jnp.minimum(sizes[donor] - 1, bound - sizes[receiver]) // 2
    slack = jnp.where((donor == order[0]) | (receiver == order[0]) | (sizes[receiver] == 0), 0, jnp.maximum(slack, 0))
    shifted = jax.random.randint(jax.random.fold_in(own, 4), (amount // 2,), 0, 1 << 20) % (slack + 1)
    sizes = sizes.at[donor].add(-shifted).at[receiver].add(shifted)
    labels = jnp.searchsorted(jnp.cumsum(sizes), jnp.arange(rows * top), side="right").astype(jnp.int32)
    table = labels.reshape(top, rows).T
    table = table[jax.random.permutation(jax.random.fold_in(own, 1), rows)]
    offset_by = jax.random.randint(jax.random.fold_in(own, 2), (rows, 1), 0, top)
    return jnp.take_along_axis(table, (jnp.arange(top)[None, :] + offset_by) % top, axis=1)


def load_shares(amount, total, reach, skew, full):
    portions = [(1 << 20) // math.isqrt(grade ** skew) + 1 for grade in range(1, amount + 1)]
    largest = reach if full else min(reach, max(-(-total // amount), total * portions[0] // sum(portions)))
    least = 1 if total - largest >= amount - 1 else 0
    counts, spare = [largest] + [least] * (amount - 1), total - largest - least * (amount - 1)
    while spare > 0:
        candidates = [i for i in range(1, amount) if counts[i] < largest] or [i for i in range(1, amount) if counts[i] < reach]
        whole, left = sum([portions[i] for i in candidates]), spare
        for i in candidates:
            more = min(reach - counts[i], max(1, left * portions[i] // whole), spare)
            counts[i] = counts[i] + more
            spare = spare - more
    return np.array(counts)


def noise(stream_key, shape, scale, most, cuts=(), kind=jnp.bfloat16):
    values = jax.random.normal(stream_key, shape, jnp.float32) * scale
    if len(cuts) > 0:
        values = levels(stream_key, shape, cuts, -0.22, 0.18) * values
    return jnp.clip(values, min=-most, max=most).astype(kind)


def setup_inputs(seed: int = 0, part: int = 0) -> dict:
    splits = jax.random.split(jax.random.key(seed), 13)
    own_keys = jax.random.split(jax.random.fold_in(splits[12], part), 13)
    a_tokens = noise(own_keys[0], (TA, D), 1.0, 6.0, ((0, 128),))
    a_gain = jnp.clip(1.0 + 0.15 * jax.random.normal(splits[1], (D,), jnp.float32), 0.25, 1.75)
    dense_gate = noise(splits[2], (D, FF), D ** -0.5, 0.0625, ((1, 128),))
    dense_up = noise(splits[3], (D, FF), D ** -0.5, 0.0625, ((1, 128),))
    dense_down = noise(splits[4], (FF, D), FF ** -0.5, 0.046875, ((0, 128),))
    b_tokens = noise(own_keys[5], (TB, D), 1.0, 6.0, ((0, 128),))
    b_gain = jnp.clip(1.0 + 0.15 * jax.random.normal(splits[6], (D,), jnp.float32), 0.25, 1.75)
    expert_ids_keys = jax.random.split(jax.random.fold_in(own_keys[7], 1), TB // TB_DEV)
    expert_ids_turns = jax.random.permutation(jax.random.fold_in(own_keys[7], 3), TB // TB_DEV)
    expert_ids = jax.vmap(lambda own, number: shared_out(jax.random.fold_in(own_keys[7], 2), own, number, TB_DEV, EXPERTS, TOPK, CAP, 2))(expert_ids_keys, expert_ids_turns).reshape((TB, TOPK))
    route_weights = jnp.clip(jnp.exp(math.log(0.5) - 2.3025851 * jax.random.uniform(own_keys[8], (TB, TOPK), jnp.float32) ** levels(own_keys[8], (TB, TOPK), ((0, 128),), -0.2, 0.2)), 0.05, 0.5)
    expert_gate = noise(splits[9], (EXPERTS * GROUP, D, ES), D ** -0.5, 0.0625, ((0, 128),))
    expert_up = noise(splits[10], (EXPERTS * GROUP, D, ES), D ** -0.5, 0.0625, ((0, 128),))
    expert_down = noise(splits[11], (EXPERTS * GROUP, ES, D), EH ** -0.5, 0.1875, ((0, 128),))
    return dict(a_tokens=a_tokens, a_gain=a_gain, dense_gate=dense_gate, dense_up=dense_up, dense_down=dense_down, b_tokens=b_tokens, b_gain=b_gain, expert_ids=expert_ids, route_weights=route_weights, expert_gate=expert_gate, expert_up=expert_up, expert_down=expert_down)


def normed(values, gain_vec):
    return values * lax.rsqrt(lax.optimization_barrier(jnp.mean(values * values, axis=-1, keepdims=True)) + 1e-06) * gain_vec

def reference(a_tokens, a_gain, dense_gate, dense_up, dense_down, b_tokens, b_gain, expert_ids, route_weights, expert_gate, expert_up, expert_down):
    a_float = a_tokens.astype(jnp.float32)
    a_normed = normed(a_float, a_gain).astype(jnp.bfloat16)
    gate_proj = jnp.dot(a_normed, dense_gate, preferred_element_type=jnp.float32)
    up_proj = jnp.dot(a_normed, dense_up, preferred_element_type=jnp.float32)
    hidden = (jax.nn.silu(gate_proj) * up_proj).astype(jnp.bfloat16)
    a_out = (a_float + jnp.dot(hidden, dense_down, preferred_element_type=jnp.float32)).astype(jnp.bfloat16)
    b_float = b_tokens.astype(jnp.float32)
    b_normed = normed(b_float, b_gain).astype(jnp.bfloat16)
    b_wide = b_normed.astype(jnp.float32)
    onehot = (expert_ids[:, :, None] == jnp.arange(EXPERTS, dtype=jnp.int32)[None, None, :]).astype(jnp.float32)
    mix_table = jnp.einsum('tk,tke->et', route_weights.astype(jnp.float32), onehot)
    gate_blocks = expert_gate.reshape(EXPERTS, GROUP, D, ES)
    up_blocks = expert_up.reshape(EXPERTS, GROUP, D, ES)
    down_blocks = expert_down.reshape(EXPERTS, GROUP, ES, D)

    def one_expert(running, inputs):
        w_gate, w_up, w_down, weight = inputs
        gate_e = jnp.einsum('td,gds->tgs', b_wide, w_gate.astype(jnp.float32))
        up_e = jnp.einsum('td,gds->tgs', b_wide, w_up.astype(jnp.float32))
        hid_e = (jax.nn.silu(gate_e) * up_e).astype(jnp.bfloat16)
        partial_value = jnp.einsum('tgs,gsd->tgd', hid_e.astype(jnp.float32), w_down.astype(jnp.float32)).astype(jnp.bfloat16)
        expert_out = lax.optimization_barrier(jnp.sum(partial_value.astype(jnp.float32), axis=1)).astype(jnp.bfloat16)
        return (running + weight[:, None] * expert_out.astype(jnp.float32), None)
    totals, _ = lax.scan(one_expert, jnp.zeros((TB, D), jnp.float32), (gate_blocks, up_blocks, down_blocks, mix_table))
    b_out = (b_float + totals).astype(jnp.bfloat16)
    return (a_out, b_out)
```

```python
import functools

import jax
import jax.numpy as jnp
from jax import lax
from jax.experimental import pallas as pl
from jax.experimental.pallas import tpu as pltpu
from jax.sharding import Mesh
from jax.sharding import PartitionSpec as P

EXPERTS = 16
REP_EXP = ("rep", "exp_0", "exp_1", "exp_2")
EXP = ("exp_0", "exp_1", "exp_2")
LONG = ("exp_1", "exp_0")
SHORT = ("exp_0", "exp_1")
BF16 = jnp.bfloat16
F32 = jnp.float32
MESH = pl.DeviceIdType.MESH
UNIT = 16


def iota2(rows, columns):
    shape = (rows, columns)
    return lax.broadcasted_iota(jnp.int32, shape, 0), lax.broadcasted_iota(jnp.int32, shape, 1)


def ones_where(condition):
    return jnp.where(condition, 1.0, 0.0).astype(BF16)


def silu(values):
    return values / (1.0 + jnp.exp(-values))


def kernel(
    n, u_ref, wg_hbm, wu_hbm, wd_hbm, eg_hbm, eu_hbm, ed_hbm, out_ref,
    xu, xa, xb, wg, wu, wd, egu, ed, acc_a, acc_b, oa, ob, pa, pb, ra, rb, yu, zu,
    w_sem, s1, r1, sa, ra_sem, sb, rb_sem, spa, rpa, spb, rpb,
    ta, qa, tb, qb, tpa, qpa, tpb, qpb, s2, r2,
):
    depth = wg.shape[0]
    half = depth // 2
    quarter = depth // 4
    wide = xb.shape[-1]
    block = 2 * n
    core = lax.axis_index("exp_2")
    other = 1 - core
    place = [lax.axis_index(LONG[0]), lax.axis_index(LONG[1])]
    spot = [place[1], place[0]]
    expert = ((lax.axis_index("exp_0") * n + lax.axis_index("exp_1")) * 2 + core) // (
        2 * n * n // EXPERTS
    )

    def along(position, distance):
        return lax.rem(position + distance + n, n)

    weights = [
        pltpu.make_async_copy(wg_hbm, wg, w_sem.at[0]),
        pltpu.make_async_copy(wu_hbm, wu, w_sem.at[1]),
        pltpu.make_async_copy(wd_hbm, wd, w_sem.at[2]),
        pltpu.make_async_copy(eg_hbm, egu.at[:, pl.ds(0, eg_hbm.shape[1])], w_sem.at[3]),
        pltpu.make_async_copy(
            eu_hbm, egu.at[:, pl.ds(eg_hbm.shape[1], eu_hbm.shape[1])], w_sem.at[4]
        ),
        pltpu.make_async_copy(ed_hbm, ed, w_sem.at[5]),
    ]
    for copy in weights:
        copy.start()

    barrier = pltpu.get_barrier_semaphore()
    pl.semaphore_signal(barrier, inc=1, device_id={"exp_2": other}, device_id_type=MESH)
    for h in range(2):
        for k in range(1, n):
            pl.semaphore_signal(
                barrier, inc=1, device_id={SHORT[h]: along(spot[h], k)}, device_id_type=MESH
            )
    pl.semaphore_wait(barrier, 2 * (n - 1) + 1)

    first = []
    for k in sorted(range(1, n), key=lambda k: -min(k, n - k)):
        for h in range(2):
            copy = pltpu.make_async_remote_copy(
                src_ref=u_ref.at[h], dst_ref=xu.at[h, spot[h]],
                send_sem=s1.at[h, k], recv_sem=r1.at[h, k],
                device_id={SHORT[h]: along(spot[h], k)}, device_id_type=MESH,
            )
            copy.start()
            first.append(copy)
    for h in range(2):
        xu[h, spot[h]] = u_ref[h]
    for copy in first:
        copy.wait()

    gathered = ((xa, sa, ra_sem, spa, rpa), (xb, sb, rb_sem, spb, rpb))
    half_cut = ((pl.ds(0, quarter), pl.ds(quarter, half - quarter)),
                (pl.ds(0, half), pl.ds(half, wide - half)))

    def hop(which, h, d, t, origin):
        ref, send, recv = gathered[which][:3]
        view = ref.at[h, core, origin]
        if t == n // 2:
            view = ref.at[h, core, origin, :, half_cut[which][d]]
        return pltpu.make_async_remote_copy(
            src_ref=view, dst_ref=view, send_sem=send.at[h, d, t - 1], recv_sem=recv.at[h, d, t - 1],
            device_id={LONG[h]: along(place[h], 1 - 2 * d)}, device_id_type=MESH,
        )

    def share(which, h, slot_core, origin, k):
        ref, _, _, send, recv = gathered[which]
        view = ref.at[h, slot_core, origin]
        return pltpu.make_async_remote_copy(
            src_ref=view, dst_ref=view, send_sem=send.at[h, k], recv_sem=recv.at[h, k],
            device_id={"exp_2": other}, device_id_type=MESH,
        )

    i, j = iota2(7 * block, UNIT * n)
    spread = ones_where(
        (j // UNIT == lax.rem(i, block) // 2)
        & (lax.rem(j, UNIT) == 2 * (i // block) + lax.rem(i, 2))
    )
    for h in range(2):
        pieces = jnp.dot(
            spread, xu[h].reshape(n * UNIT, quarter), preferred_element_type=F32
        ).astype(BF16)
        for g in range(2):
            xa[h, core, place[h], :, pl.ds(g * quarter, quarter)] = pieces[
                g * block : (g + 1) * block
            ]
        for g in range(4):
            xb[h, core, place[h], :, pl.ds(g * quarter, quarter)] = pieces[
                (g + 2) * block : (g + 3) * block
            ]
        xb[h, core, place[h], :, pl.ds(depth, wide - depth)] = pieces[
            6 * block : 7 * block, : wide - depth
        ]
    sent = []
    for which in range(2):
        for h in range(2):
            for d in range(2):
                copy = hop(which, h, d, 1, place[h])
                copy.start()
                sent.append(copy)
        for h in range(2):
            copy = share(which, h, core, place[h], 0)
            copy.start()
            sent.append(copy)
    for t in range(1, n // 2 + 1):
        for which in range(2):
            for h in range(2):
                for d in range(2):
                    origin = along(place[h], -t * (1 - 2 * d))
                    hop(which, h, d, t, origin).wait_recv()
                    if t < n // 2:
                        copy = hop(which, h, d, t + 1, origin)
                        copy.start()
                        sent.append(copy)
                        copy = share(which, h, core, origin, 2 * t - 1 + d)
                        copy.start()
                        sent.append(copy)
                    elif d == 1:
                        copy = share(which, h, core, origin, n - 1)
                        copy.start()
                        sent.append(copy)

    def arrivals(which):
        for h in range(2):
            for k in range(n):
                t = (k + 1) // 2
                origin = along(place[h], -t * (1 - 2 * ((k + 1) % 2)))
                share(which, h, other, origin, k).wait_recv()

    for copy in weights:
        copy.wait()

    arrivals(0)
    rows_a = 4 * n * n
    i, j = iota2(rows_a, rows_a)
    within = lax.rem(i, 2 * n * n)
    swap = ones_where(
        j == i - within + (lax.rem(within, block) // 2) * block + (within // block) * 2 + lax.rem(i, 2)
    )
    chunk = min(512, quarter)
    acc_a[...] = jnp.zeros_like(acc_a)

    def dense_in(k, carry):
        low = pl.ds(pl.multiple_of(k * chunk, chunk), chunk)
        high = pl.ds(pl.multiple_of(k * chunk + half, chunk), chunk)
        x0 = xa[0, :, :, :, low].reshape(rows_a, chunk)
        x1 = xa[1, :, :, :, low].reshape(rows_a, chunk)
        x1 = jnp.dot(swap, x1, preferred_element_type=F32).astype(BF16)
        for p, w in enumerate((wg, wu)):
            acc_a[p] += jnp.dot(x0, w[low, :], preferred_element_type=F32) + jnp.dot(
                x1, w[high, :], preferred_element_type=F32
            )
        return carry

    lax.fori_loop(0, half // chunk, dense_in, 0)
    hidden = (silu(acc_a[0]) * acc_a[1]).astype(BF16)
    hidden_swapped = jnp.dot(swap, hidden, preferred_element_type=F32).astype(BF16)

    def dense_out(k, carry):
        low = pl.ds(pl.multiple_of(k * chunk, chunk), chunk)
        high = pl.ds(pl.multiple_of(k * chunk + half, chunk), chunk)
        for h, (rows, columns) in enumerate(((hidden, low), (hidden_swapped, high))):
            oa[h, :, :, :, low] = (
                jnp.dot(rows, wd[:, columns], preferred_element_type=F32)
                .astype(BF16)
                .reshape(2, n, block, chunk)
            )
        return carry

    lax.fori_loop(0, half // chunk, dense_out, 0)

    arrivals(1)
    rows_b = 8 * n * n
    acc_b[...] = jnp.zeros_like(acc_b)

    def expert_in(k, carry):
        low = pl.ds(pl.multiple_of(k * chunk, chunk), chunk)
        x = xb[:, :, :, :, low].reshape(rows_b, chunk)
        acc_b[...] += jnp.dot(x, egu[low, :], preferred_element_type=F32)
        return carry

    lax.fori_loop(0, depth // chunk, expert_in, 0)
    units = egu.shape[1] // 2
    hidden = (silu(acc_b[:, :units]) * acc_b[:, units:]).astype(BF16)
    table = xb[:, :, :, :, pl.ds(depth, wide - depth)].reshape(rows_b, wide - depth).astype(F32)
    _, lane = iota2(rows_b, wide - depth)
    weight = jnp.sum(
        jnp.where((lane == expert) | (lane == expert + EXPERTS), table, 0.0), axis=1, keepdims=True
    )

    def expert_out(k, carry):
        low = pl.ds(pl.multiple_of(k * chunk, chunk), chunk)
        ob[:, :, :, :, low] = (
            (jnp.dot(hidden, ed[:, low], preferred_element_type=F32) * weight)
            .astype(BF16)
            .reshape(2, 2, n, block, chunk)
        )
        return carry

    lax.fori_loop(0, depth // chunk, expert_out, 0)

    reduced = ((oa, pa, ra, ta, qa, tpa, qpa), (ob, pb, rb, tb, qb, tpb, qpb))
    cut = ((pl.ds(0, quarter), pl.ds(quarter, quarter)), (pl.ds(0, half), pl.ds(half, half)))

    def give(which, h, k):
        ref, theirs, _, _, _, send, recv = reduced[which]
        return pltpu.make_async_remote_copy(
            src_ref=ref.at[h, other, along(place[h], n // 2 + k)],
            dst_ref=theirs.at[h, along(place[h], n // 2 + k)],
            send_sem=send.at[h, k], recv_sem=recv.at[h, k],
            device_id={"exp_2": other}, device_id_type=MESH,
        )

    def pass_on(which, h, d, t):
        ref, _, ring, send, recv = reduced[which][:5]
        slot = along(place[h], (n // 2 + 1 - t) * (1 - 2 * d))
        source, target = ref.at[h, core, slot], ring.at[h, d, t - 1]
        if t == 1:
            source = ref.at[h, core, slot, :, cut[which][d]]
            target = ring.at[h, d, 0, :, cut[which][d]]
        return pltpu.make_async_remote_copy(
            src_ref=source, dst_ref=target, send_sem=send.at[h, d, t - 1], recv_sem=recv.at[h, d, t - 1],
            device_id={LONG[h]: along(place[h], 1 - 2 * d)}, device_id_type=MESH,
        )

    def give_order():
        order = [0]
        for t in range(1, n // 2):
            order += [n - t, t]
        return order + [n // 2]

    for k in give_order():
        for which in range(2):
            for h in range(2):
                copy = give(which, h, k)
                copy.start()
                sent.append(copy)
    for t in range(1, n // 2 + 1):
        for which in range(2):
            ref, theirs, ring = reduced[which][:3]
            for h in range(2):
                if t == 1:
                    give(which, h, 0).wait_recv()
                for d in range(2):
                    sign = 1 - 2 * d
                    slot = along(place[h], (n // 2 + 1 - t) * sign)
                    if t == 1:
                        part = cut[which][d]
                        ref[h, core, slot, :, part] = (
                            ref[h, core, slot, :, part].astype(F32)
                            + theirs[h, slot, :, part].astype(F32)
                        ).astype(BF16)
                    else:
                        give(which, h, (n + (1 - t) * sign) % n).wait_recv()
                        pass_on(which, h, d, t - 1).wait_recv()
                        if t == 2:
                            for p in range(2):
                                part = cut[which][p]
                                total = ref[h, core, slot, :, part].astype(F32) + theirs[
                                    h, slot, :, part
                                ].astype(F32)
                                if p == d:
                                    total += ring[h, d, 0, :, part].astype(F32)
                                ref[h, core, slot, :, part] = total.astype(BF16)
                        else:
                            ref[h, core, slot] = (
                                ref[h, core, slot].astype(F32)
                                + theirs[h, slot].astype(F32)
                                + ring[h, d, t - 2].astype(F32)
                            ).astype(BF16)
                    copy = pass_on(which, h, d, t)
                    copy.start()
                    sent.append(copy)

    i, j = iota2(UNIT * n, 6 * block)
    collect = ones_where(
        (i // UNIT == lax.rem(j, block) // 2)
        & (lax.rem(i, UNIT) == 2 * (j // block) + lax.rem(j, 2))
    )
    last = []
    for h in range(2):
        totals = []
        for which in range(2):
            ref, theirs, ring = reduced[which][:3]
            give(which, h, n // 2).wait_recv()
            total = ref[h, core, place[h]].astype(F32) + theirs[h, place[h]].astype(F32)
            for d in range(2):
                pass_on(which, h, d, n // 2).wait_recv()
                total += ring[h, d, n // 2 - 1].astype(F32)
            totals.append(total.astype(BF16))
        stack = jnp.concatenate(
            [totals[0][:, g * quarter : (g + 1) * quarter] for g in range(2)]
            + [totals[1][:, g * quarter : (g + 1) * quarter] for g in range(4)],
            axis=0,
        )
        yu[h] = (
            jnp.dot(collect, stack, preferred_element_type=F32)
            .astype(BF16)
            .reshape(n, UNIT, quarter)
        )
        for k in sorted(range(1, n), key=lambda k: -min(k, n - k)):
            copy = pltpu.make_async_remote_copy(
                src_ref=yu.at[h, along(spot[h], k)], dst_ref=zu.at[h, k],
                send_sem=s2.at[h, k], recv_sem=r2.at[h, k],
                device_id={SHORT[h]: along(spot[h], k)}, device_id_type=MESH,
            )
            copy.start()
            last.append(copy)
    for copy in last:
        copy.wait_recv()
    for h in range(2):
        total = yu[h, spot[h]].astype(F32)
        for k in range(1, n):
            total += zu[h, k].astype(F32)
        out_ref[h] = total
    for copy in sent + last:
        copy.wait_send()


def layers(units, dense_gate, dense_up, dense_down, expert_gate, expert_up, expert_down):
    n = lax.axis_size("exp_0")
    depth, hidden = dense_gate.shape
    expert_hidden = expert_gate.shape[1]
    half, quarter, wide, block = depth // 2, depth // 4, depth + 128, 2 * n
    hops = n // 2
    dma = pltpu.SemaphoreType.DMA
    scratch = [
        pltpu.VMEM((2, n, UNIT, quarter), BF16),
        pltpu.VMEM((2, 2, n, block, half), BF16),
        pltpu.VMEM((2, 2, n, block, wide), BF16),
        pltpu.VMEM((depth, hidden), BF16),
        pltpu.VMEM((depth, hidden), BF16),
        pltpu.VMEM((hidden, depth), BF16),
        pltpu.VMEM((depth, 2 * expert_hidden), BF16),
        pltpu.VMEM((expert_hidden, depth), BF16),
        pltpu.VMEM((2, 4 * n * n, hidden), F32),
        pltpu.VMEM((8 * n * n, 2 * expert_hidden), F32),
        pltpu.VMEM((2, 2, n, block, half), BF16),
        pltpu.VMEM((2, 2, n, block, depth), BF16),
        pltpu.VMEM((2, n, block, half), BF16),
        pltpu.VMEM((2, n, block, depth), BF16),
        pltpu.VMEM((2, 2, hops, block, half), BF16),
        pltpu.VMEM((2, 2, hops, block, depth), BF16),
        pltpu.VMEM((2, n, UNIT, quarter), BF16),
        pltpu.VMEM((2, n, UNIT, quarter), BF16),
        dma((6,)),
        dma((2, n)), dma((2, n)),
        dma((2, 2, hops)), dma((2, 2, hops)), dma((2, 2, hops)), dma((2, 2, hops)),
        dma((2, n)), dma((2, n)), dma((2, n)), dma((2, n)),
        dma((2, 2, hops)), dma((2, 2, hops)), dma((2, 2, hops)), dma((2, 2, hops)),
        dma((2, n)), dma((2, n)), dma((2, n)), dma((2, n)),
        dma((2, n)), dma((2, n)),
    ]
    vmem = pl.BlockSpec(memory_space=pltpu.VMEM)
    anywhere = pl.BlockSpec(memory_space=pl.ANY)
    return pl.pallas_call(
        functools.partial(kernel, n),
        out_shape=jax.ShapeDtypeStruct((2, UNIT, quarter), F32),
        in_specs=[vmem] + [anywhere] * 6,
        out_specs=vmem,
        scratch_shapes=scratch,
        compiler_params=pltpu.CompilerParams(
            collective_id=0, has_side_effects=True, vmem_limit_bytes=64 * 1024 * 1024 - 65536
        ),
    )(units, dense_gate, dense_up, dense_down, expert_gate, expert_up, expert_down)


def normed(values, gain_vec):
    return values * lax.rsqrt(jnp.mean(values * values, axis=-1, keepdims=True) + 1e-06) * gain_vec


def shards(
    a_tokens,
    a_gain,
    dense_gate,
    dense_up,
    dense_down,
    b_tokens,
    b_gain,
    expert_ids,
    route_weights,
    expert_gate,
    expert_up,
    expert_down,
):
    depth = a_tokens.shape[1]
    quarter = depth // 4
    a_float = a_tokens.astype(F32)
    b_float = b_tokens.astype(F32)
    a_normed = normed(a_float, a_gain).astype(BF16)
    b_normed = normed(b_float, b_gain).astype(BF16)
    onehot = (expert_ids[:, :, None] == jnp.arange(EXPERTS, dtype=jnp.int32)).astype(F32)
    table = jnp.sum(route_weights[:, :, None] * onehot, axis=1)
    high = lax.reduce_precision(table, 8, 7)
    table = jnp.concatenate([high, table - high], axis=1).astype(BF16)
    table = jnp.pad(table, ((0, 0), (0, quarter - table.shape[1]))).reshape(2, 1, 2, quarter)
    a_unit = a_normed.reshape(2, 2, 2, quarter).transpose(1, 2, 0, 3)
    b_unit = b_normed.reshape(2, 2, 4, quarter).transpose(0, 2, 1, 3)
    empty = jnp.zeros((2, 1, 2, quarter), BF16)
    units = jnp.concatenate([a_unit, b_unit, table, empty], axis=1).reshape(2, UNIT, quarter)
    sums = layers(
        units, dense_gate, dense_up, dense_down, expert_gate[0], expert_up[0], expert_down[0]
    )
    sums = sums.reshape(2, UNIT // 2, 2, quarter)
    a_sum = sums[:, 0:2].transpose(2, 0, 1, 3).reshape(a_tokens.shape)
    b_sum = sums[:, 2:6].transpose(0, 2, 1, 3).reshape(b_tokens.shape)
    return ((a_float + a_sum).astype(BF16), (b_float + b_sum).astype(BF16))


def solution(mesh):
    finer = Mesh(
        mesh.devices.reshape(mesh.shape["rep"], 8, 8, 2), ("rep", "exp_0", "exp_1", "exp_2")
    )
    placed = (
        P(REP_EXP, None),
        P(),
        P(None, EXP),
        P(None, EXP),
        P(EXP, None),
        P(REP_EXP, None),
        P(),
        P(REP_EXP, None),
        P(REP_EXP, None),
        P(EXP, None, None),
        P(EXP, None, None),
        P(EXP, None, None),
    )
    return jax.shard_map(
        shards,
        mesh=finer,
        in_specs=placed,
        out_specs=(P(REP_EXP, None), P(REP_EXP, None)),
        check_vma=False,
    )
```

```python
import functools

import jax
import jax.numpy as jnp
from jax import lax
from jax.experimental import pallas as pl
from jax.experimental.pallas import tpu as pltpu
from jax.sharding import Mesh
from jax.sharding import PartitionSpec as P

EXPERTS = 16
REP_EXP = ("rep", "exp_0", "exp_1", "exp_2")
EXP = ("exp_0", "exp_1", "exp_2")
LONG = ("exp_1", "exp_0")
SHORT = ("exp_0", "exp_1")
BF16 = jnp.bfloat16
F32 = jnp.float32
MESH = pl.DeviceIdType.MESH
UNIT = 16


def iota2(rows, columns):
    shape = (rows, columns)
    return lax.broadcasted_iota(jnp.int32, shape, 0), lax.broadcasted_iota(jnp.int32, shape, 1)


def ones_where(condition):
    return jnp.where(condition, 1.0, 0.0).astype(BF16)


def silu(values):
    return values / (1.0 + jnp.exp(-values))


def unit_place(i, n):
    j = i - 4 * n
    device = jnp.where(i < 4 * n, lax.rem(i, n), lax.rem(j, 2 * n) // 2)
    row = jnp.where(i < 4 * n, i // n, 4 + 2 * (j // (2 * n)) + lax.rem(j, 2))
    return device, row


def transposed_dot(rows, weight):
    return lax.dot_general(rows, weight, (((1,), (1,)), ((), ())), preferred_element_type=F32)


def kernel(
    n, a_ref, ag_ref, b_ref, bg_ref, ids_ref, route_ref,
    wg_hbm, wu_hbm, wd_hbm, eg_hbm, eu_hbm, ed_hbm, a_out, b_out,
    uf, u, xu, xa, xb, wg, wu, wd, egu, ed, acc_a, acc_b, oa, ob, pa, pb, ra, rb, yu, zu,
    a_sum, b_sum,
    w_sem, s1, r1, sa, ra_sem, sb, rb_sem, spa, rpa, spb, rpb,
    ta, qa, tb, qb, tpa, qpa, tpb, qpb, s2, r2,
):
    depth = a_ref.shape[1]
    half = depth // 2
    quarter = depth // 4
    wide = xb.shape[-1]
    last = n // 2
    core = lax.axis_index("exp_2")
    other = 1 - core
    place = [lax.axis_index(LONG[0]), lax.axis_index(LONG[1])]
    spot = [place[1], place[0]]
    expert = ((lax.axis_index("exp_0") * n + lax.axis_index("exp_1")) * 2 + core) // (
        2 * n * n // EXPERTS
    )

    def along(position, distance):
        return lax.rem(position + distance + n, n)

    barrier = pltpu.get_barrier_semaphore()
    pl.semaphore_signal(barrier, inc=1, device_id={"exp_2": other}, device_id_type=MESH)
    for h in range(2):
        for k in range(1, n):
            pl.semaphore_signal(
                barrier, inc=1, device_id={SHORT[h]: along(spot[h], k)}, device_id_type=MESH
            )

    units = eg_hbm.shape[1]
    weights = [
        pltpu.make_async_copy(wg_hbm, wg, w_sem.at[0]),
        pltpu.make_async_copy(wu_hbm, wu, w_sem.at[1]),
        pltpu.make_async_copy(wd_hbm, wd, w_sem.at[2]),
        pltpu.make_async_copy(eg_hbm, egu.at[:, pl.ds(0, units)], w_sem.at[3]),
        pltpu.make_async_copy(eu_hbm, egu.at[:, pl.ds(units, units)], w_sem.at[4]),
        pltpu.make_async_copy(ed_hbm, ed, w_sem.at[5]),
    ]
    for copy in weights:
        copy.start()

    a_float = a_ref[...].astype(F32)
    b_float = b_ref[...].astype(F32)
    a_normed = normed(a_float, ag_ref[...])
    b_normed = normed(b_float, bg_ref[...])
    uf[...] = jnp.zeros_like(uf)
    _, lane = iota2(b_ref.shape[0], wide - depth)
    table = jnp.zeros(lane.shape, F32)
    for k in range(ids_ref.shape[1]):
        hit = (lax.rem(lane, EXPERTS) == ids_ref[:, k : k + 1]) & (lane < 2 * EXPERTS)
        table += jnp.where(hit, route_ref[:, k : k + 1], 0.0)
    high = table.astype(BF16).astype(F32)
    table = jnp.where(lane < EXPERTS, high, table - high)
    for h in range(2):
        for g in range(4):
            part = slice(g * quarter, (g + 1) * quarter)
            uf[h, g : g + 1] = a_normed[h : h + 1, part]
            uf[h, 4 + 2 * g : 6 + 2 * g] = b_normed[2 * h : 2 * h + 2, part]
        uf[h, 12:14, 0 : wide - depth] = table[2 * h : 2 * h + 2]
    u[...] = uf[...].astype(BF16)

    pl.semaphore_wait(barrier, 2 * (n - 1) + 1)

    first = []
    for k in sorted(range(1, n), key=lambda k: -min(k, n - k)):
        for h in range(2):
            copy = pltpu.make_async_remote_copy(
                src_ref=u.at[h], dst_ref=xu.at[h, spot[h]],
                send_sem=s1.at[h, k], recv_sem=r1.at[h, k],
                device_id={SHORT[h]: along(spot[h], k)}, device_id_type=MESH,
            )
            copy.start()
            first.append(copy)
    for h in range(2):
        xu[h, spot[h]] = u[h]
    i, j = iota2(14 * n, UNIT * n)
    device, row = unit_place(i, n)
    spread = ones_where(j == device * UNIT + row)
    i, j = iota2(UNIT * n, 12 * n)
    device, row = unit_place(j, n)
    collect = ones_where(i == device * UNIT + row)
    for copy in first:
        copy.wait()

    gathered = ((xa, sa, ra_sem, spa, rpa), (xb, sb, rb_sem, spb, rpb))
    half_cut = ((pl.ds(0, half), pl.ds(half, half)),
                (pl.ds(0, half), pl.ds(half, wide - half)))
    sent = []

    def start(copy):
        copy.start()
        sent.append(copy)

    def hop(which, h, d, t, origin):
        ref, send, recv = gathered[which][:3]
        view = ref.at[h, core, origin]
        if t == last:
            view = ref.at[h, core, origin, :, half_cut[which][d]]
        return pltpu.make_async_remote_copy(
            src_ref=view, dst_ref=view, send_sem=send.at[h, d, t - 1], recv_sem=recv.at[h, d, t - 1],
            device_id={LONG[h]: along(place[h], 1 - 2 * d)}, device_id_type=MESH,
        )

    def share(which, h, slot_core, origin, k):
        ref, _, _, send, recv = gathered[which]
        view = ref.at[h, slot_core, origin]
        return pltpu.make_async_remote_copy(
            src_ref=view, dst_ref=view, send_sem=send.at[h, k], recv_sem=recv.at[h, k],
            device_id={"exp_2": other}, device_id_type=MESH,
        )

    for h in range(2):
        pieces = jnp.dot(
            spread, xu[h].reshape(n * UNIT, quarter), preferred_element_type=F32
        )
        for g in range(4):
            part = pl.ds(g * quarter, quarter)
            xa[h, core, place[h], :, part] = pieces[g * n : (g + 1) * n].astype(BF16)
            xb[h, core, place[h], :, part] = pieces[
                (4 + 2 * g) * n : (6 + 2 * g) * n
            ].astype(BF16)
        xb[h, core, place[h], :, pl.ds(depth, wide - depth)] = pieces[
            12 * n : 14 * n, : wide - depth
        ].astype(BF16)
    for which in range(2):
        for h in range(2):
            for d in range(2):
                start(hop(which, h, d, 1, place[h]))
        for h in range(2):
            start(share(which, h, core, place[h], 0))

    def steps(t):
        if t == 0:
            return [(h, 0, 0) for h in range(2)]
        if t == last:
            return [(h, last, n - 1) for h in range(2)]
        return [(h, t * (2 * d - 1), 2 * t - 1 + d) for h in range(2) for d in range(2)]

    def blocks_of(t):
        return [(h, c, along(place[h], s)) for h, s, _ in steps(t) for c in (core, other)]

    reduced = ((oa, pa, ra, ta, qa, tpa, qpa), (ob, pb, rb, tb, qb, tpb, qpb))
    cut = (pl.ds(0, half), pl.ds(half, half))

    def give(which, h, slot, k):
        ref, theirs, _, _, _, send, recv = reduced[which]
        return pltpu.make_async_remote_copy(
            src_ref=ref.at[h, other, slot], dst_ref=theirs.at[h, slot],
            send_sem=send.at[h, k], recv_sem=recv.at[h, k],
            device_id={"exp_2": other}, device_id_type=MESH,
        )

    chunk = min(1024, quarter)

    def layer(which, t):
        for h, s, k in steps(t):
            share(which, h, other, along(place[h], s), k).wait_recv()
        if t == 0:
            for copy in weights[3 * which : 3 * which + 3]:
                copy.wait()
        blocks = blocks_of(t)
        rows = (n, 2 * n)[which] * len(blocks)
        each = rows // len(blocks)

        def span(k):
            return pl.ds(pl.multiple_of(k * chunk, chunk), chunk)

        if which == 0:
            for p in range(2):
                acc_a[p, :rows] = jnp.zeros((rows, acc_a.shape[2]), F32)

            def dense_in(k, carry):
                x = jnp.concatenate(
                    [xa[h, c, slot, :, span(k)].astype(F32) for h, c, slot in blocks], axis=0
                ).astype(BF16)
                for p, w in enumerate((wg, wu)):
                    acc_a[p, :rows] += transposed_dot(x, w[:, span(k)])
                return carry

            lax.fori_loop(0, depth // chunk, dense_in, 0)
            hidden = (silu(acc_a[0, :rows]) * acc_a[1, :rows]).astype(BF16)

            def dense_out(k, carry):
                y = jnp.dot(hidden, wd[:, span(k)], preferred_element_type=F32)
                for i, (h, c, slot) in enumerate(blocks):
                    oa[h, c, slot, :, span(k)] = y[i * each : (i + 1) * each].astype(BF16)
                return carry

            lax.fori_loop(0, depth // chunk, dense_out, 0)
        else:
            acc_b[:rows] = jnp.zeros((rows, acc_b.shape[1]), F32)

            def expert_in(k, carry):
                x = jnp.concatenate([xb[h, c, slot, :, span(k)] for h, c, slot in blocks], axis=0)
                acc_b[:rows] += jnp.dot(x, egu[span(k), :], preferred_element_type=F32)
                return carry

            lax.fori_loop(0, depth // chunk, expert_in, 0)
            hidden = (silu(acc_b[:rows, :units]) * acc_b[:rows, units:]).astype(BF16)
            table = jnp.concatenate(
                [xb[h, c, slot, :, pl.ds(depth, wide - depth)] for h, c, slot in blocks], axis=0
            ).astype(F32)
            _, lane = iota2(rows, wide - depth)
            weight = jnp.sum(
                jnp.where((lane == expert) | (lane == expert + EXPERTS), table, 0.0),
                axis=1, keepdims=True,
            )

            def expert_out(k, carry):
                y = jnp.dot(hidden, ed[:, span(k)], preferred_element_type=F32) * weight
                for i, (h, c, slot) in enumerate(blocks):
                    ob[h, c, slot, :, span(k)] = y[i * each : (i + 1) * each].astype(BF16)
                return carry

            lax.fori_loop(0, depth // chunk, expert_out, 0)
        for h, s, k in steps(t):
            start(give(which, h, along(place[h], s), k))

    for t in range(1, last + 1):
        for which in range(2):
            layer(which, t - 1)
            for h in range(2):
                for d in range(2):
                    origin = along(place[h], -t * (1 - 2 * d))
                    hop(which, h, d, t, origin).wait_recv()
                    if t < last:
                        start(hop(which, h, d, t + 1, origin))
                        start(share(which, h, core, origin, 2 * t - 1 + d))
                    elif d == 1:
                        start(share(which, h, core, origin, n - 1))

    def pass_on(which, h, d, t):
        ref, _, ring, send, recv = reduced[which][:5]
        slot = along(place[h], (last + 1 - t) * (1 - 2 * d))
        source, target = ref.at[h, core, slot], ring.at[h, d, t - 1]
        if t == 1:
            source = ref.at[h, core, slot, :, cut[d]]
            target = ring.at[h, d, 0, :, cut[d]]
        return pltpu.make_async_remote_copy(
            src_ref=source, dst_ref=target, send_sem=send.at[h, d, t - 1], recv_sem=recv.at[h, d, t - 1],
            device_id={LONG[h]: along(place[h], 1 - 2 * d)}, device_id_type=MESH,
        )

    for t in range(1, last + 1):
        for which in range(2):
            ref, theirs, ring = reduced[which][:3]
            if t == 1:
                layer(which, last)
            for h in range(2):
                if t == 1:
                    give(which, h, along(place[h], last), n - 1).wait_recv()
                for d in range(2):
                    distance = last + 1 - t
                    slot = along(place[h], distance * (1 - 2 * d))
                    if t == 1:
                        ref[h, core, slot, :, cut[d]] = (
                            ref[h, core, slot, :, cut[d]].astype(F32)
                            + theirs[h, slot, :, cut[d]].astype(F32)
                        ).astype(BF16)
                    else:
                        give(which, h, slot, 2 * distance - d).wait_recv()
                        pass_on(which, h, d, t - 1).wait_recv()
                        for p in range(2):
                            total = ref[h, core, slot, :, cut[p]].astype(F32) + theirs[
                                h, slot, :, cut[p]
                            ].astype(F32)
                            if t > 2 or p == d:
                                total += ring[h, d, t - 2, :, cut[p]].astype(F32)
                            ref[h, core, slot, :, cut[p]] = total.astype(BF16)
                    start(pass_on(which, h, d, t))

    final = []
    for h in range(2):
        totals = []
        for which in range(2):
            ref, theirs, ring = reduced[which][:3]
            give(which, h, place[h], 0).wait_recv()
            total = ref[h, core, place[h]].astype(F32) + theirs[h, place[h]].astype(F32)
            for d in range(2):
                pass_on(which, h, d, last).wait_recv()
                total += ring[h, d, last - 1].astype(F32)
            totals += [total[:, g * quarter : (g + 1) * quarter] for g in range(4)]
        stack = jnp.concatenate(totals, axis=0).astype(BF16)
        yu[h] = (
            jnp.dot(collect, stack, preferred_element_type=F32)
            .astype(BF16)
            .reshape(n, UNIT, quarter)
        )
        for k in sorted(range(1, n), key=lambda k: -min(k, n - k)):
            copy = pltpu.make_async_remote_copy(
                src_ref=yu.at[h, along(spot[h], k)], dst_ref=zu.at[h, k],
                send_sem=s2.at[h, k], recv_sem=r2.at[h, k],
                device_id={SHORT[h]: along(spot[h], k)}, device_id_type=MESH,
            )
            start(copy)
            final.append(copy)
    for copy in final:
        copy.wait_recv()
    for h in range(2):
        total = yu[h, spot[h]].astype(F32)
        for k in range(1, n):
            total += zu[h, k].astype(F32)
        uf[h] = total
    for h in range(2):
        for g in range(4):
            part = pl.ds(g * quarter, quarter)
            a_sum[h : h + 1, part] = uf[h, g : g + 1]
            b_sum[2 * h : 2 * h + 2, part] = uf[h, 4 + 2 * g : 6 + 2 * g]
    a_out[...] = (a_ref[...].astype(F32) + a_sum[...]).astype(BF16)
    b_out[...] = (b_ref[...].astype(F32) + b_sum[...]).astype(BF16)
    for copy in sent:
        copy.wait_send()


def normed(values, gain_vec):
    return values * lax.rsqrt(jnp.mean(values * values, axis=-1, keepdims=True) + 1e-06) * gain_vec


def shards(
    a_tokens,
    a_gain,
    dense_gate,
    dense_up,
    dense_down,
    b_tokens,
    b_gain,
    expert_ids,
    route_weights,
    expert_gate,
    expert_up,
    expert_down,
):
    n = lax.axis_size("exp_0")
    depth, hidden = dense_gate.shape
    units = expert_gate.shape[2]
    quarter, wide = depth // 4, depth + 128
    hops = n // 2
    dma = pltpu.SemaphoreType.DMA
    scratch = [
        pltpu.VMEM((2, UNIT, quarter), F32),
        pltpu.VMEM((2, UNIT, quarter), BF16),
        pltpu.VMEM((2, n, UNIT, quarter), BF16),
        pltpu.VMEM((2, 2, n, n, depth), BF16),
        pltpu.VMEM((2, 2, n, 2 * n, wide), BF16),
        pltpu.VMEM((hidden, depth), BF16),
        pltpu.VMEM((hidden, depth), BF16),
        pltpu.VMEM((hidden, depth), BF16),
        pltpu.VMEM((depth, 2 * units), BF16),
        pltpu.VMEM((units, depth), BF16),
        pltpu.VMEM((2, 8 * n, hidden), F32),
        pltpu.VMEM((16 * n, 2 * units), F32),
        pltpu.VMEM((2, 2, n, n, depth), BF16),
        pltpu.VMEM((2, 2, n, 2 * n, depth), BF16),
        pltpu.VMEM((2, n, n, depth), BF16),
        pltpu.VMEM((2, n, 2 * n, depth), BF16),
        pltpu.VMEM((2, 2, hops, n, depth), BF16),
        pltpu.VMEM((2, 2, hops, 2 * n, depth), BF16),
        pltpu.VMEM((2, n, UNIT, quarter), BF16),
        pltpu.VMEM((2, n, UNIT, quarter), BF16),
        pltpu.VMEM(a_tokens.shape, F32),
        pltpu.VMEM(b_tokens.shape, F32),
        dma((6,)),
        dma((2, n)), dma((2, n)),
        dma((2, 2, hops)), dma((2, 2, hops)), dma((2, 2, hops)), dma((2, 2, hops)),
        dma((2, n)), dma((2, n)), dma((2, n)), dma((2, n)),
        dma((2, 2, hops)), dma((2, 2, hops)), dma((2, 2, hops)), dma((2, 2, hops)),
        dma((2, n)), dma((2, n)), dma((2, n)), dma((2, n)),
        dma((2, n)), dma((2, n)),
    ]
    vmem = pl.BlockSpec(memory_space=pltpu.VMEM)
    anywhere = pl.BlockSpec(memory_space=pl.ANY)
    return pl.pallas_call(
        functools.partial(kernel, n),
        out_shape=(
            jax.ShapeDtypeStruct(a_tokens.shape, BF16),
            jax.ShapeDtypeStruct(b_tokens.shape, BF16),
        ),
        in_specs=[vmem] * 6 + [anywhere] * 6,
        out_specs=(vmem, vmem),
        scratch_shapes=scratch,
        compiler_params=pltpu.CompilerParams(
            collective_id=0, has_side_effects=True, vmem_limit_bytes=64 * 1024 * 1024 - 65536
        ),
    )(
        a_tokens,
        a_gain[None, :],
        b_tokens,
        b_gain[None, :],
        expert_ids,
        route_weights,
        dense_gate.T,
        dense_up.T,
        dense_down,
        expert_gate[0],
        expert_up[0],
        expert_down[0],
    )


def solution(mesh):
    finer = Mesh(
        mesh.devices.reshape(mesh.shape["rep"], 8, 8, 2), ("rep", "exp_0", "exp_1", "exp_2")
    )
    placed = (
        P(REP_EXP, None),
        P(),
        P(None, EXP),
        P(None, EXP),
        P(EXP, None),
        P(REP_EXP, None),
        P(),
        P(REP_EXP, None),
        P(REP_EXP, None),
        P(EXP, None, None),
        P(EXP, None, None),
        P(EXP, None, None),
    )
    return jax.shard_map(
        shards,
        mesh=finer,
        in_specs=placed,
        out_specs=(P(REP_EXP, None), P(REP_EXP, None)),
        check_vma=False,
    )
```
